128 devices in a mesh: rep: 1, dp: 128 (over x, y, z, core).
Axes of the slice: x: 4, y: 4, z: 4, core: 2. Of those that a mesh axis runs over, the one named last changes fastest.
Arguments:
- x: bfloat16 [128, 1024, 896], P(('rep', 'dp'))
- dy: bfloat16 [128, 1024, 896], P(('rep', 'dp'))
- w_gate: bfloat16 [2, 896, 2304], replicated
- w_up: bfloat16 [2, 896, 2304], replicated
- w_down: bfloat16 [2, 2304, 896], replicated
- m_w_gate: float32 [2, 896, 2304], replicated
- m_w_up: float32 [2, 896, 2304], replicated
- m_w_down: float32 [2, 2304, 896], replicated
- v_w_gate: float32 [2, 896, 2304], replicated
- v_w_up: float32 [2, 896, 2304], replicated
- v_w_down: float32 [2, 2304, 896], replicated
Outputs:
- output 1: bfloat16 [2, 896, 2304], P('rep')
- output 2: bfloat16 [2, 896, 2304], P('rep')
- output 3: bfloat16 [2, 2304, 896], P('rep')
- output 4: float32 [2, 896, 2304], P('rep')
- output 5: float32 [2, 896, 2304], P('rep')
- output 6: float32 [2, 2304, 896], P('rep')
- output 7: float32 [2, 896, 2304], P('rep')
- output 8: float32 [2, 896, 2304], P('rep')
- output 9: float32 [2, 2304, 896], P('rep')
All inputs are finite; a program needn't handle non-finite values.
Results may differ from the reference program's by a relative error of at most 0.022.
Values are sent between devices in bfloat16 or wider.
A program may use at most 1.5 GiB of HBM per device.

```python
import jax
import jax.numpy as jnp
from jax import lax

SEQUENCES = 128
TOKENS = 1024
D = 896
FF = 2304
LAYERS = 2
NAMES = ("w_gate", "w_up", "w_down")
SHAPES = {"w_gate": (LAYERS, D, FF), "w_up": (LAYERS, D, FF), "w_down": (LAYERS, FF, D)}


def bump(key, n, height):
    away = (jnp.arange(n, dtype=jnp.int32) - jax.random.randint(key, (), 0, n, jnp.int32)) % n
    return jnp.where(away < n // 8, height, 1.0)


def together(key, own, strength):
    shared = jax.random.normal(key, own.shape[1:], jnp.float32)
    return (own + strength * shared) * lax.rsqrt(1 + strength * strength)


def setup_inputs(seed: int = 0, part: int = 0) -> dict:
    kx, kdy, ka, kb, kz, kf, kh, kl, *keys = jax.random.split(jax.random.key(seed), 8 + 3 * len(NAMES))
    kx, kdy, ka, kb = (jax.random.fold_in(k, part) for k in (kx, kdy, ka, kb))
    kw, km, kv = (keys[i::3] for i in range(3))
    shape = (SEQUENCES, TOKENS, D)
    much_x, much_dy = jax.random.uniform(kz, (2,), jnp.float32, 0.0, 1.0)
    loud = 2.0 ** jax.random.uniform(jax.random.fold_in(kz, 1), (), jnp.float32, -1.0, 2.0)
    layers = 2.0 ** jax.random.uniform(kl, (LAYERS, 1, 1), jnp.float32, -1.0, 1.0)
    x = together(ka, jax.random.normal(kx, shape, jnp.float32), much_x) * bump(kf, D, 4.0)
    dy = together(kb, jax.random.normal(kdy, shape, jnp.float32), much_dy)
    drawn = {"x": x.astype(jnp.bfloat16), "dy": (loud * dy * (SEQUENCES * TOKENS) ** -0.5).astype(jnp.bfloat16)}
    for key, name in zip(kw, NAMES, strict=True):
        w = jax.random.normal(key, SHAPES[name], jnp.float32) * SHAPES[name][1] ** -0.5
        drawn[name] = (w * {"w_gate": 1.0, "w_up": bump(kh, FF, 4.0), "w_down": layers}[name]).astype(jnp.bfloat16)
    for key, name in zip(km, NAMES, strict=True):
        drawn[f"m_{name}"] = 0.1 * jax.random.normal(key, SHAPES[name], jnp.float32)
    for key, name in zip(kv, NAMES, strict=True):
        drawn[f"v_{name}"] = jax.random.uniform(key, SHAPES[name], jnp.float32, 0.005, 0.015)
    return drawn


def matmul(a, w):
    return jnp.dot(a, w, preferred_element_type=jnp.float32).astype(jnp.bfloat16)


def normed(h):
    wide = h.astype(jnp.float32)
    scale = lax.rsqrt(jnp.mean(wide**2, -1, keepdims=True) + 1e-6)
    return (wide * scale).astype(jnp.bfloat16)


def layer(h, w):
    a = normed(h)
    gate = jnp.dot(a, w["w_gate"], preferred_element_type=jnp.float32)
    up = jnp.dot(a, w["w_up"], preferred_element_type=jnp.float32)
    return h + matmul((jax.nn.silu(gate) * up).astype(jnp.bfloat16), w["w_down"])


def adamw(w, m, v, g):
    m = 0.9 * m + 0.1 * g
    v = 0.95 * v + 0.05 * g * g
    step = m * lax.rsqrt(v + 1e-8) + 0.1 * w
    return (w - 0.02 * step).astype(jnp.bfloat16), m, v


def clipped(gradients, sum_of_squares, count):
    factor = jnp.minimum(1.0, 0.5 * lax.rsqrt(sum_of_squares / count + 1e-30))
    return [g * factor for g in gradients]


def stack(weights, h):
    return lax.scan(lambda h, w: (layer(h, w), None), h, weights)[0]


def reference(x, dy, w_gate, w_up, w_down, m_w_gate, m_w_up, m_w_down, v_w_gate, v_w_up, v_w_down):
    weights = dict(zip(NAMES, (w_gate, w_up, w_down), strict=True))

    def take(so_far, sequence):
        h, by_y = sequence
        _, back = jax.vjp(lambda w: stack(w, h), weights)
        return jax.tree.map(lambda total, term: total + term.astype(jnp.float32), so_far, back(by_y)[0]), None

    none_yet = {name: jnp.zeros(w.shape, jnp.float32) for name, w in weights.items()}
    by_weights, _ = lax.scan(take, none_yet, (x, dy))
    gradients = [by_weights[name].astype(jnp.bfloat16).astype(jnp.float32) for name in NAMES]
    gradients = clipped(gradients, sum(jnp.sum(g * g) for g in gradients), sum(g.size for g in gradients))
    new = [
        adamw(w.astype(jnp.float32), m, v, g)
        for w, m, v, g in zip((w_gate, w_up, w_down), (m_w_gate, m_w_up, m_w_down), (v_w_gate, v_w_up, v_w_down), gradients, strict=True)
    ]
    return tuple(one[which] for which in range(3) for one in new)
```

```python
import functools

import jax
import jax.numpy as jnp
from jax import lax
from jax.experimental import pallas as pl
from jax.experimental.pallas import tpu as pltpu
from jax.sharding import PartitionSpec as P

NAMES = ("w_gate", "w_up", "w_down")
BF, F32 = jnp.bfloat16, jnp.float32
BLOCK = ((56, 1152), (56, 1152), (72, 896))
UPWARD = 32
AXES = ((0, 1, 2), (1, 2, 0), (2, 0, 1))


class Sems:
    def __init__(self, ref):
        self.ref, self.used = ref, 0

    def __call__(self):
        self.used += 1
        return self.ref.at[self.used - 1]


def reduce_kernel(*refs):
    ins = [[refs[l * 3 + k] for k in range(3)] for l in range(2)]
    outs, ss_out = refs[6:9], refs[9]
    it = iter(refs[10:-3])
    own, far, q1, q2, via, f, t, v1, v2, uvia, x, fin = ([[next(it) for _ in range(3)] for _ in range(2)] for _ in range(12))
    ss, ssx, sem_ref = refs[-3:]
    sem = Sems(sem_ref)

    me = lax.axis_index("dp")
    core = lax.rem(me, 2)
    pos = [lax.rem(me // 32, 4), lax.rem(me // 8, 4), lax.rem(me // 2, 4)]
    stride = (32, 8, 2)

    def at(axis, by):
        return me + (lax.rem(pos[axis] + by + 4, 4) - pos[axis]) * stride[axis]

    partner = me + 1 - 2 * core

    def dev(index):
        return (0, index)

    def part(ref, k, half, first, n, rows=slice(None)):
        if k < 2:
            return ref.at[pl.ds(first, n), rows, pl.ds(pl.multiple_of(half * 1152, 128), 1152)]
        return ref.at[pl.ds(half * 16 + first, n), rows, :]

    pending = []

    def send(src, dst, to):
        copy = pltpu.make_async_remote_copy(
            src_ref=src, dst_ref=dst, send_sem=sem(), recv_sem=sem(), device_id=dev(to), device_id_type=pl.DeviceIdType.MESH
        )
        copy.start()
        pending.append(copy)
        return copy

    barrier = pltpu.get_barrier_semaphore()
    friends = [partner] + [at(a, by) for a in range(3) for by in (1, 2, 3)]
    for friend in friends:
        pl.semaphore_signal(barrier, inc=1, device_id=dev(friend), device_id_type=pl.DeviceIdType.MESH)
    pl.semaphore_wait(barrier, len(friends))

    got = {}

    def blocks(n, body):
        lax.fori_loop(0, n, lambda i, c: (body(i), c)[1], 0)

    def wide(ref, i):
        return ref[i].astype(F32)

    def s0(l, by):
        for k in range(3):
            p = pos[AXES[k][0]]
            first = lax.rem(p + by, 4) * 4
            copy = pltpu.make_async_copy(part(ins[l][k], k, core, first, 4), own[l][k].at[pl.ds(first, 4)], sem())
            copy.start()
            got[l, k, "own", by] = copy
            got[l, k, "far", by] = send(part(ins[l][k], k, 1 - core, first, 4), far[l][k].at[pl.ds(first, 4)], partner)

    def both(l, k, by):
        got[l, k, "own", by].wait()
        got[l, k, "far", by].wait_recv()

    def presum(l, k, first, n):
        def body(i):
            own[l][k][first + i] = (wide(own[l][k], first + i) + wide(far[l][k], first + i)).astype(BF)

        blocks(n, body)

    def s1(l, k):
        a = AXES[k][0]
        p = pos[a]
        both(l, k, 2)
        b = lax.rem(p + 2, 4) * 4
        presum(l, k, b, 4)
        got[l, k, "1p"] = send(own[l][k].at[pl.ds(b, 2)], via[l][k].at[0], at(a, 1))
        got[l, k, "1m"] = send(own[l][k].at[pl.ds(b + 2, 2)], via[l][k].at[1], at(a, 3))

    def s2(l, k):
        a = AXES[k][0]
        p = pos[a]
        both(l, k, 1)
        b = lax.rem(p + 1, 4) * 4 + 2
        presum(l, k, b, 2)
        got[l, k, "2p"] = send(own[l][k].at[pl.ds(b, 2)], q1[l][k].at[pl.ds(2, 2)], at(a, 1))
        both(l, k, 3)
        b = lax.rem(p + 3, 4) * 4
        presum(l, k, b, 2)
        got[l, k, "2m"] = send(own[l][k].at[pl.ds(b, 2)], q1[l][k].at[pl.ds(0, 2)], at(a, 3))

    def s3(l, k):
        a = AXES[k][0]
        p = pos[a]
        for way, by, half in ((0, 1, 0), (1, 3, 2)):
            got[l, k, "1pm"[0] + "pm"[way]].wait_recv()
            b = lax.rem(p + by, 4) * 4 + half

            def body(i):
                own[l][k][b + i] = (wide(own[l][k], b + i) + wide(far[l][k], b + i) + via[l][k][way, i].astype(F32)).astype(BF)

            blocks(2, body)
            got[l, k, "3" + "pm"[way]] = send(own[l][k].at[pl.ds(b, 2)], q2[l][k].at[pl.ds(half, 2)], at(a, by))

    up, down = slice(0, UPWARD), slice(UPWARD, None)

    def s4(l, k):
        a, a2 = AXES[k][:2]
        p, q = pos[a], pos[a2]
        both(l, k, 0)
        for name in ("2p", "2m", "3p", "3m"):
            got[l, k, name].wait_recv()

        def body(i):
            j = lax.rem(q + 2 + i, 4)
            whole = wide(own[l][k], p * 4 + j) + wide(far[l][k], p * 4 + j) + wide(q1[l][k], j) + wide(q2[l][k], j)
            f[l][k][i] = whole
            t[l][k][i] = whole.astype(BF)

        blocks(4, body)
        got[l, k, "u1p"] = send(t[l][k].at[0, up], uvia[l][k].at[up], at(a2, 1))
        got[l, k, "u1m"] = send(t[l][k].at[0, down], uvia[l][k].at[down], at(a2, 3))
        got[l, k, "u2p"] = send(t[l][k].at[3, down], v1[l][k].at[down], at(a2, 1))
        got[l, k, "u2m"] = send(t[l][k].at[1, up], v1[l][k].at[up], at(a2, 3))

    def s5(l, k):
        a2 = AXES[k][1]
        got[l, k, "u1p"].wait_recv()
        t[l][k][3, up] = (f[l][k][3, up] + uvia[l][k][up].astype(F32)).astype(BF)
        got[l, k, "u3p"] = send(t[l][k].at[3, up], v2[l][k].at[up], at(a2, 1))
        got[l, k, "u1m"].wait_recv()
        t[l][k][1, down] = (f[l][k][1, down] + uvia[l][k][down].astype(F32)).astype(BF)
        got[l, k, "u3m"] = send(t[l][k].at[1, down], v2[l][k].at[down], at(a2, 3))

    def s6(l, k):
        a3 = AXES[k][2]
        r = pos[a3]
        for name in ("u2p", "u2m", "u3p", "u3m"):
            got[l, k, name].wait_recv()
        x[l][k][r] = (f[l][k][2] + v1[l][k][...].astype(F32) + v2[l][k][...].astype(F32)).astype(BF)
        got[l, k, "x1p"] = send(x[l][k].at[r], x[l][k].at[r], at(a3, 1))
        got[l, k, "x1m"] = send(x[l][k].at[r], x[l][k].at[r], at(a3, 3))

    def s7(l, k):
        a3 = AXES[k][2]
        r = pos[a3]
        got[l, k, "x1p"].wait_recv()
        b = lax.rem(r + 3, 4)
        got[l, k, "x2p"] = send(x[l][k].at[b, up], x[l][k].at[b, up], at(a3, 1))
        got[l, k, "x1m"].wait_recv()
        b = lax.rem(r + 1, 4)
        got[l, k, "x2m"] = send(x[l][k].at[b, down], x[l][k].at[b, down], at(a3, 3))

    def place(l, k, half, first, n, rows=slice(None)):
        return part(outs[k].at[l], k, half, first, n, rows)

    def s8(l, k):
        a, a2 = AXES[k][:2]
        p, q = pos[a], pos[a2]
        got[l, k, "x2p"].wait_recv()
        got[l, k, "x2m"].wait_recv()
        whole = (x[l][k][0].astype(F32) + x[l][k][1].astype(F32)) + (x[l][k][2].astype(F32) + x[l][k][3].astype(F32))
        g = whole.astype(BF)
        fin[l][k][0] = g
        mine = p * 4 + q
        copy = pltpu.make_async_copy(fin[l][k], place(l, k, core, mine, 1), sem())
        copy.start()
        got[l, k, "mine"] = copy
        got[l, k, "y1p"] = send(fin[l][k], place(l, k, core, mine, 1), at(a2, 1))
        got[l, k, "y1m"] = send(fin[l][k], place(l, k, core, mine, 1), at(a2, 3))
        got[l, k, "z1p", 0] = send(fin[l][k], place(l, k, core, mine, 1), at(a, 1))
        got[l, k, "z1m", 0] = send(fin[l][k], place(l, k, core, mine, 1), at(a, 3))
        wide_g = g.astype(F32)
        squares = wide_g * wide_g
        rows, cols = BLOCK[k]
        by_row = sum(squares[i : i + 8] for i in range(0, rows, 8))
        return sum(by_row[:, i : i + 128] for i in range(0, cols, 128))

    def s9(l, k):
        a, a2 = AXES[k][:2]
        p, q = pos[a], pos[a2]
        for name, by, rows, to in (("p", 3, up, 1), ("m", 1, down, 3)):
            got[l, k, "y1" + name].wait_recv()
            b = p * 4 + lax.rem(q + by, 4)
            got[l, k, "y2" + name] = send(place(l, k, core, b, 1, rows), place(l, k, core, b, 1, rows), at(a2, to))
            for way, ahead in (("p", 1), ("m", 3)):
                got[l, k, "z1" + way, by] = send(place(l, k, core, b, 1), place(l, k, core, b, 1), at(a, ahead))

    def onward(l, k, d):
        a, a2 = AXES[k][:2]
        p, q = pos[a], pos[a2]
        j = lax.rem(q + d, 4)
        for name, by, rows, to in (("p", 3, up, 1), ("m", 1, down, 3)):
            got[l, k, "z1" + name, d].wait_recv()
            b = lax.rem(p + by, 4) * 4 + j
            got[l, k, "z2" + name, d] = send(place(l, k, core, b, 1, rows), place(l, k, core, b, 1, rows), at(a, to))

    def s10(l, k):
        a, a2 = AXES[k][:2]
        p, q = pos[a], pos[a2]
        got[l, k, "y2p"].wait_recv()
        got[l, k, "y2m"].wait_recv()
        b = p * 4 + lax.rem(q + 2, 4)
        for way, ahead in (("p", 1), ("m", 3)):
            got[l, k, "z1" + way, 2] = send(place(l, k, core, b, 1), place(l, k, core, b, 1), at(a, ahead))
        got[l, k, "mine"].wait()
        got[l, k, "c", 0] = send(place(l, k, core, p * 4, 4), place(l, k, core, p * 4, 4), partner)
        onward(l, k, 0)

    def s11(l, k):
        for d in (3, 1, 2):
            onward(l, k, d)
        p = pos[AXES[k][0]]
        for by in (1, 3):
            b = lax.rem(p + by, 4) * 4
            got[l, k, "c", by] = send(place(l, k, core, b, 4), place(l, k, core, b, 4), partner)

    def s12(l, k):
        for d in range(4):
            got[l, k, "z2p", d].wait_recv()
            got[l, k, "z2m", d].wait_recv()
        b = lax.rem(pos[AXES[k][0]] + 2, 4) * 4
        got[l, k, "c", 2] = send(place(l, k, core, b, 4), place(l, k, core, b, 4), partner)

    def run(stage, l):
        return [stage(l, k) for k in range(3)]

    for l in (1, 0):
        for by in (2, 1, 3, 0):
            s0(l, by)
    run(s1, 1)
    run(s2, 1)
    run(s3, 1)
    run(s1, 0)
    run(s2, 0)
    run(s4, 1)
    run(s5, 1)
    run(s3, 0)
    run(s6, 1)
    run(s7, 1)
    run(s4, 0)
    sums = run(s8, 1)
    run(s5, 0)
    run(s9, 1)
    run(s6, 0)
    run(s7, 0)
    run(s10, 1)
    sums += run(s8, 0)

    total = sum(sums)
    here = []
    for number, (count, spot, others) in enumerate(
        [(2, core, [(partner, 1)])] + [(4, pos[a], [(at(a, by), by) for by in (1, 2, 3)]) for a in range(3)]
    ):
        ss[number] = total
        ssx[number, spot] = total
        arrivals = [send(ss.at[number], ssx.at[number, spot], to) for to, _ in others]
        here.append((count, arrivals))
        if number == 0:
            run(s9, 0)
        elif number == 1:
            run(s10, 0)
        elif number == 2:
            run(s11, 1)
        for arrival in arrivals:
            arrival.wait_recv()
        total = ssx[number, 0] + ssx[number, 1]
        if count == 4:
            total = total + (ssx[number, 2] + ssx[number, 3])
    ss_out[...] = total

    run(s12, 1)
    run(s11, 0)
    run(s12, 0)
    for l in (1, 0):
        for k in range(3):
            for by in range(4):
                got[l, k, "c", by].wait_recv()
    for copy in pending:
        copy.wait_send()


def summed(layers):
    scratch = []
    per = lambda shape, dtype: [pltpu.VMEM(shape(*BLOCK[k]), dtype) for _ in range(2) for k in range(3)]
    for shape, dtype in (
        (lambda r, c: (16, r, c), BF),
        (lambda r, c: (16, r, c), BF),
        (lambda r, c: (4, r, c), BF),
        (lambda r, c: (4, r, c), BF),
        (lambda r, c: (2, 2, r, c), BF),
        (lambda r, c: (4, r, c), F32),
        (lambda r, c: (4, r, c), BF),
        (lambda r, c: (r, c), BF),
        (lambda r, c: (r, c), BF),
        (lambda r, c: (r, c), BF),
        (lambda r, c: (4, r, c), BF),
        (lambda r, c: (1, r, c), BF),
    ):
        scratch += per(shape, dtype)
    scratch += [pltpu.VMEM((4, 8, 128), F32), pltpu.VMEM((4, 4, 8, 128), F32), pltpu.SemaphoreType.DMA((640,))]
    blocked = [[g.reshape(-1, BLOCK[k][0], g.shape[-1]) for k, g in enumerate(layer)] for layer in layers]
    outs = [jax.ShapeDtypeStruct((2, *g.shape), BF) for g in blocked[0]]
    *sums, squares = pl.pallas_call(
        reduce_kernel,
        out_shape=[*outs, jax.ShapeDtypeStruct((8, 128), F32)],
        in_specs=[pl.BlockSpec(memory_space=pltpu.HBM)] * 6,
        out_specs=[pl.BlockSpec(memory_space=pltpu.HBM)] * 3 + [pl.BlockSpec(memory_space=pltpu.VMEM)],
        scratch_shapes=scratch,
        compiler_params=pltpu.CompilerParams(collective_id=0, has_side_effects=True, vmem_limit_bytes=66_000_000),
    )(*blocked[0], *blocked[1])
    return [s.reshape(2, *g.shape) for s, g in zip(sums, layers[0], strict=True)], jnp.sum(squares)


def matmul(a, w):
    return jnp.dot(a, w, preferred_element_type=jnp.float32).astype(jnp.bfloat16)


def normed(h):
    wide = h.astype(jnp.float32)
    scale = lax.rsqrt(jnp.mean(wide**2, -1, keepdims=True) + 1e-6)
    return (wide * scale).astype(jnp.bfloat16)


def layer(h, w):
    a = normed(h)
    gate = jnp.dot(a, w["w_gate"], preferred_element_type=jnp.float32)
    up = jnp.dot(a, w["w_up"], preferred_element_type=jnp.float32)
    return h + matmul((jax.nn.silu(gate) * up).astype(jnp.bfloat16), w["w_down"])


def adamw(w, m, v, g):
    m = 0.9 * m + 0.1 * g
    v = 0.95 * v + 0.05 * g * g
    step = m * lax.rsqrt(v + 1e-8) + 0.1 * w
    return (w - 0.02 * step).astype(jnp.bfloat16), m, v


def clipped(gradients, sum_of_squares, count):
    factor = jnp.minimum(1.0, 0.5 * lax.rsqrt(sum_of_squares / count + 1e-30))
    return [g * factor for g in gradients]


def solution(mesh):
    def step(x, dy, *arrays):
        weights, m, v = (arrays[i : i + 3] for i in (0, 3, 6))
        layers = weights[0].shape[0]
        h, kept = x[0], []
        for number in range(layers):
            kept.append(h)
            h = layer(h, {name: w[number] for name, w in zip(NAMES, weights, strict=True)})
        by_h, terms = dy[0], [None] * layers
        for number in reversed(range(layers)):
            _, back = jax.vjp(lambda w, h: layer(h, w), {name: w[number] for name, w in zip(NAMES, weights, strict=True)}, kept[number])
            by_w, by_h = back(by_h)
            terms[number] = [by_w[name] for name in NAMES]
        gradients, squares = summed(terms)
        gradients = [g.astype(jnp.float32) for g in gradients]
        gradients = clipped(gradients, 0.25 * squares, sum(g.size for g in gradients))
        new = [adamw(w.astype(jnp.float32), m, v, g) for w, m, v, g in zip(weights, m, v, gradients, strict=True)]
        return tuple(one[which] for which in range(3) for one in new)

    return jax.shard_map(
        step,
        mesh=mesh,
        in_specs=(P(("rep", "dp"), None, None),) * 2 + (P(None, None, None),) * 9,
        out_specs=(P("rep", None, None),) * 9,
        check_vma=False,
    )
```

```python
import functools

import jax
import jax.numpy as jnp
from jax import lax
from jax.experimental import pallas as pl
from jax.experimental.pallas import tpu as pltpu
from jax.sharding import PartitionSpec as P

BF, F32 = jnp.bfloat16, jnp.float32
UNITS = ((0, 0, 56, 640), (0, 640, 56, 512), (1, 0, 56, 640), (1, 640, 56, 512), (2, 0, 72, 512), (2, 512, 72, 384))
AXES = ((0, 1, 2), (1, 2, 0), (2, 0, 1)) * 2
UPWARD = 32
SLOT = 4.2
GAPS = (4, 4, 4, 3.5, 4, 4, 5, 6)


class Sems:
    def __init__(self, ref):
        self.ref, self.used = ref, 0

    def __call__(self):
        self.used += 1
        return self.ref.at[self.used - 1]


def reduce_kernel(*refs):
    ins = [refs[l * 5 : l * 5 + 5] for l in range(2)]
    outs, ss_out = refs[10:13], refs[13]
    it = iter(refs[14:-7])
    own, far, q1, q2, via, v1, v2, uvia, x, fin = ([[next(it) for _ in UNITS] for _ in range(2)] for _ in range(10))
    f, t, theirs = ([each] * 2 for each in ([next(it) for _ in UNITS] for _ in range(3)))
    tall, broad, deep, flat, ss, ssx, sem_ref = refs[-7:]
    sem = Sems(sem_ref)

    me = lax.axis_index("dp")
    core = lax.rem(me, 2)
    pos = [lax.rem(me // 32, 4), lax.rem(me // 8, 4), lax.rem(me // 2, 4)]
    stride = (32, 8, 2)

    def turn(place, by):
        return lax.rem(place + by, 4)

    def at(axis, by):
        return me + (turn(pos[axis], by) - pos[axis]) * stride[axis]

    partner = me + 1 - 2 * core

    def dev(index):
        return (0, index)

    def part(ref, k, half, first, n, rows=slice(None)):
        matrix, column, _, width = UNITS[k]
        if matrix == 2:
            return ref.at[pl.ds(half * 16 + first, n), rows, pl.ds(column, width)]
        return ref.at[pl.ds(first, n), rows, pl.ds(pl.multiple_of(half * 1152 + column, 128), width)]

    pending = []

    def remote(src, dst, to, send_sem, recv_sem):
        return pltpu.make_async_remote_copy(
            src_ref=src, dst_ref=dst, send_sem=send_sem, recv_sem=recv_sem, device_id=dev(to), device_id_type=pl.DeviceIdType.MESH
        )

    def send(src, dst, to):
        copy = remote(src, dst, to, sem(), sem())
        copy.start()
        pending.append(copy)
        return copy

    friends = [partner] + [at(a, by) for a in range(3) for by in (1, 2, 3)]

    def sent(copy):
        copy.wait_send()
        pending[:] = [each for each in pending if each is not copy]

    got = {}
    order = [(l, k) for l in (1, 0) for k in range(len(UNITS))]

    def blocks(n, body):
        lax.fori_loop(0, n, lambda i, c: (body(i), c)[1], 0)

    def wide(ref, i):
        return ref[i].astype(F32)

    loads = {}

    def load(name, l, which, dst):
        loads[name, l] = pltpu.make_async_copy(ins[l][which], dst, sem())
        loads[name, l].start()

    def s0(l, k):
        matrix, column, rows, width = UNITS[k]
        if not column:
            for name in (("tall", "gate"), ("up",), ("deep", "flat"))[matrix]:
                loads[name, l].wait()
        if l == 0:
            for by in range(4):
                sent(got[1, k, "far", by])
        base = sem.used
        sem.used += 8

        def fourth(by):
            some = pl.ds(turn(pos[AXES[k][0]], by) * 4, 4)
            return remote(theirs[l][k].at[some], far[l][k].at[some], partner, sem.ref.at[base + by], sem.ref.at[base + 4 + by])

        def body(i):
            by = turn(i, 2)
            first = turn(pos[AXES[k][0]], by) * 4
            for half, to in ((1 - core, theirs[l][k]), (core, own[l][k])):
                if matrix == 2:
                    lhs = deep[pl.ds(pl.multiple_of(half * 1152 + first * rows, 8), 4 * rows), :]
                    rhs = flat[:, column : column + width]
                else:
                    lhs = tall[pl.ds(pl.multiple_of(first * rows, 8), 4 * rows), :]
                    rhs = broad[:, pl.ds(pl.multiple_of(half * 1152 + column, 128), width)]
                to[pl.ds(first, 4)] = jnp.dot(lhs, rhs, preferred_element_type=F32).reshape(4, rows, width).astype(BF)
                if to is theirs[l][k]:
                    fourth(by).start()

        blocks(4, body)
        for by in range(4):
            got[l, k, "far", by] = fourth(by)
            pending.append(got[l, k, "far", by])
        if column:
            if matrix == 0:
                load("up", l, 2, broad)
            elif l == 1 and matrix == 1:
                load("tall", 0, 0, tall)
                load("gate", 0, 1, broad)
            elif l == 1:
                load("deep", 0, 3, deep)
                load("flat", 0, 4, flat)

    def both(l, k, by):
        got[l, k, "far", by].wait_recv()

    def presum(l, k, first, n):
        def body(i):
            own[l][k][first + i] = (wide(own[l][k], first + i) + wide(far[l][k], first + i)).astype(BF)

        blocks(n, body)

    def s1(l, k):
        a = AXES[k][0]
        p = pos[a]
        both(l, k, 2)
        b = turn(p, 2) * 4
        presum(l, k, b, 4)
        got[l, k, "1p"] = send(own[l][k].at[pl.ds(b, 2)], via[l][k].at[0], at(a, 1))
        got[l, k, "1m"] = send(own[l][k].at[pl.ds(b + 2, 2)], via[l][k].at[1], at(a, 3))

    def s2(l, k):
        a = AXES[k][0]
        p = pos[a]
        both(l, k, 1)
        b = turn(p, 1) * 4 + 2
        presum(l, k, b, 2)
        got[l, k, "2p"] = send(own[l][k].at[pl.ds(b, 2)], q1[l][k].at[pl.ds(2, 2)], at(a, 1))
        both(l, k, 3)
        b = turn(p, 3) * 4
        presum(l, k, b, 2)
        got[l, k, "2m"] = send(own[l][k].at[pl.ds(b, 2)], q1[l][k].at[pl.ds(0, 2)], at(a, 3))

    def s3(l, k):
        a = AXES[k][0]
        p = pos[a]
        for way, by, half in ((0, 1, 0), (1, 3, 2)):
            got[l, k, "1" + "pm"[way]].wait_recv()
            b = turn(p, by) * 4 + half

            def body(i):
                own[l][k][b + i] = (wide(own[l][k], b + i) + wide(far[l][k], b + i) + via[l][k][way, i].astype(F32)).astype(BF)

            blocks(2, body)
            got[l, k, "3" + "pm"[way]] = send(own[l][k].at[pl.ds(b, 2)], q2[l][k].at[pl.ds(half, 2)], at(a, by))

    up, down = slice(0, UPWARD), slice(UPWARD, None)
    aheads = (("p", 1), ("m", 3))
    ways = (("p", 3, up, 1), ("m", 1, down, 3))

    def s4(l, k):
        a, a2 = AXES[k][:2]
        p, q = pos[a], pos[a2]
        both(l, k, 0)
        for name in ("2p", "2m", "3p", "3m"):
            got[l, k, name].wait_recv()

        def body(i):
            j = turn(q, 2 + i)
            whole = wide(own[l][k], p * 4 + j) + wide(far[l][k], p * 4 + j) + wide(q1[l][k], j) + wide(q2[l][k], j)
            f[l][k][i] = whole
            t[l][k][i] = whole.astype(BF)

        if l == 0:
            for name in ("u1p", "u1m", "u2p", "u2m", "u3p", "u3m"):
                sent(got[1, k, name])

        blocks(4, body)
        got[l, k, "u1p"] = send(t[l][k].at[0, up], uvia[l][k].at[up], at(a2, 1))
        got[l, k, "u1m"] = send(t[l][k].at[0, down], uvia[l][k].at[down], at(a2, 3))
        got[l, k, "u2p"] = send(t[l][k].at[3, down], v1[l][k].at[down], at(a2, 1))
        got[l, k, "u2m"] = send(t[l][k].at[1, up], v1[l][k].at[up], at(a2, 3))

    def s5(l, k):
        a2 = AXES[k][1]
        got[l, k, "u1p"].wait_recv()
        t[l][k][3, up] = (f[l][k][3, up] + uvia[l][k][up].astype(F32)).astype(BF)
        got[l, k, "u3p"] = send(t[l][k].at[3, up], v2[l][k].at[up], at(a2, 1))
        got[l, k, "u1m"].wait_recv()
        t[l][k][1, down] = (f[l][k][1, down] + uvia[l][k][down].astype(F32)).astype(BF)
        got[l, k, "u3m"] = send(t[l][k].at[1, down], v2[l][k].at[down], at(a2, 3))

    def s6(l, k):
        a3 = AXES[k][2]
        r = pos[a3]
        for name in ("u2p", "u2m", "u3p", "u3m"):
            got[l, k, name].wait_recv()
        x[l][k][r] = (f[l][k][2] + v1[l][k][...].astype(F32) + v2[l][k][...].astype(F32)).astype(BF)
        got[l, k, "x1p"] = send(x[l][k].at[r], x[l][k].at[r], at(a3, 1))
        got[l, k, "x1m"] = send(x[l][k].at[r], x[l][k].at[r], at(a3, 3))

    def s7(l, k):
        a3 = AXES[k][2]
        r = pos[a3]
        got[l, k, "x1p"].wait_recv()
        b = turn(r, 3)
        got[l, k, "x2p"] = send(x[l][k].at[b, up], x[l][k].at[b, up], at(a3, 1))
        got[l, k, "x1m"].wait_recv()
        b = turn(r, 1)
        got[l, k, "x2m"] = send(x[l][k].at[b, down], x[l][k].at[b, down], at(a3, 3))

    def place(l, k, half, first, n, rows=slice(None)):
        return part(outs[UNITS[k][0]].at[l], k, half, first, n, rows)

    def s8(l, k):
        a, a2 = AXES[k][:2]
        p, q = pos[a], pos[a2]
        got[l, k, "x2p"].wait_recv()
        got[l, k, "x2m"].wait_recv()
        whole = (x[l][k][0].astype(F32) + x[l][k][1].astype(F32)) + (x[l][k][2].astype(F32) + x[l][k][3].astype(F32))
        g = whole.astype(BF)
        fin[l][k][0] = g
        mine = p * 4 + q
        copy = pltpu.make_async_copy(fin[l][k], place(l, k, core, mine, 1), sem())
        copy.start()
        got[l, k, "mine"] = copy
        got[l, k, "y1p"] = send(fin[l][k], place(l, k, core, mine, 1), at(a2, 1))
        got[l, k, "y1m"] = send(fin[l][k], place(l, k, core, mine, 1), at(a2, 3))
        got[l, k, "z1p", 0] = send(fin[l][k], place(l, k, core, mine, 1), at(a, 1))
        got[l, k, "z1m", 0] = send(fin[l][k], place(l, k, core, mine, 1), at(a, 3))
        wide_g = g.astype(F32)
        squares = wide_g * wide_g
        _, _, rows, cols = UNITS[k]
        by_row = sum(squares[i : i + 8] for i in range(0, rows, 8))
        return sum(by_row[:, i : i + 128] for i in range(0, cols, 128))

    def s9(l, k):
        a, a2 = AXES[k][:2]
        p, q = pos[a], pos[a2]
        for name, by, rows, to in ways:
            got[l, k, "y1" + name].wait_recv()
            b = p * 4 + turn(q, by)
            got[l, k, "y2" + name] = send(place(l, k, core, b, 1, rows), place(l, k, core, b, 1, rows), at(a2, to))
            for way, ahead in aheads:
                got[l, k, "z1" + way, by] = send(place(l, k, core, b, 1), place(l, k, core, b, 1), at(a, ahead))

    def onward(l, k, d):
        a, a2 = AXES[k][:2]
        p, q = pos[a], pos[a2]
        j = turn(q, d)
        for name, by, rows, to in ways:
            got[l, k, "z1" + name, d].wait_recv()
            b = turn(p, by) * 4 + j
            got[l, k, "z2" + name, d] = send(place(l, k, core, b, 1, rows), place(l, k, core, b, 1, rows), at(a, to))

    def s10(l, k):
        a, a2 = AXES[k][:2]
        p, q = pos[a], pos[a2]
        got[l, k, "y2p"].wait_recv()
        got[l, k, "y2m"].wait_recv()
        b = p * 4 + turn(q, 2)
        for way, ahead in aheads:
            got[l, k, "z1" + way, 2] = send(place(l, k, core, b, 1), place(l, k, core, b, 1), at(a, ahead))
        got[l, k, "mine"].wait()
        got[l, k, "c", 0] = send(place(l, k, core, p * 4, 4), place(l, k, core, p * 4, 4), partner)
        onward(l, k, 0)

    def s11(l, k):
        for d in (3, 1, 2):
            onward(l, k, d)
        p = pos[AXES[k][0]]
        for by in (1, 3):
            b = turn(p, by) * 4
            got[l, k, "c", by] = send(place(l, k, core, b, 4), place(l, k, core, b, 4), partner)

    def s12(l, k):
        for d in range(4):
            got[l, k, "z2p", d].wait_recv()
            got[l, k, "z2m", d].wait_recv()
        b = turn(pos[AXES[k][0]], 2) * 4
        got[l, k, "c", 2] = send(place(l, k, core, b, 4), place(l, k, core, b, 4), partner)

    rounds = [(2, core, [partner])] + [(4, pos[a], [at(a, by) for by in (1, 2, 3)]) for a in range(3)]
    squares, arrivals = [], []

    def add_squares(number):
        total = squares[-1] if number else sum(squares)
        if number:
            for arrival in arrivals.pop():
                arrival.wait_recv()
            total = ssx[number - 1, 0] + ssx[number - 1, 1]
            if number > 1:
                total = total + (ssx[number - 1, 2] + ssx[number - 1, 3])
        if number == 4:
            ss_out[...] = total
            return
        _, spot, others = rounds[number]
        ss[number] = total
        ssx[number, spot] = total
        arrivals.append([send(ss.at[number], ssx.at[number, spot], to) for to in others])

    plan = []
    for n, (l, k) in enumerate(order):
        one = SLOT * n + SLOT
        times = [SLOT * n, one, one, one + 6, one + 14]
        for gap in GAPS:
            times.append(times[-1] + gap)
        for stage, time in zip((s0, s1, s2, s3, s4, s5, s6, s7, s8, s9, s10, s11, s12), times, strict=True):
            plan.append((time, stage, (l, k)))
    last = max(time for time, stage, _ in plan if stage is s8)
    plan += [(last + 0.1 + 3 * number, add_squares, (number,)) for number in range(5)]
    for name, which, dst in (("tall", 0, tall), ("gate", 1, broad), ("deep", 3, deep), ("flat", 4, flat)):
        load(name, 1, which, dst)
    barrier = pltpu.get_barrier_semaphore()
    for friend in friends:
        pl.semaphore_signal(barrier, inc=1, device_id=dev(friend), device_id_type=pl.DeviceIdType.MESH)
    pl.semaphore_wait(barrier, len(friends))
    for _, stage, which in sorted(plan, key=lambda entry: entry[0]):
        result = stage(*which)
        if stage is s8:
            squares.append(result)
    for l, k in order:
        for by in range(4):
            got[l, k, "c", by].wait_recv()
    for copy in pending:
        copy.wait_send()


def summed(layers):
    scratch = []
    per = lambda shape, dtype, count: [pltpu.VMEM(shape(*unit[2:]), dtype) for _ in range(count) for unit in UNITS]
    for shape, dtype, count in (
        (lambda r, c: (16, r, c), BF, 2),
        (lambda r, c: (16, r, c), BF, 2),
        (lambda r, c: (4, r, c), BF, 2),
        (lambda r, c: (4, r, c), BF, 2),
        (lambda r, c: (2, 2, r, c), BF, 2),
        (lambda r, c: (r, c), BF, 2),
        (lambda r, c: (r, c), BF, 2),
        (lambda r, c: (r, c), BF, 2),
        (lambda r, c: (4, r, c), BF, 2),
        (lambda r, c: (1, r, c), BF, 2),
        (lambda r, c: (4, r, c), F32, 1),
        (lambda r, c: (4, r, c), BF, 1),
        (lambda r, c: (16, r, c), BF, 1),
    ):
        scratch += per(shape, dtype, count)
    a, by_gate, _, act, by_out = layers[0]
    scratch += [pltpu.VMEM(a.shape, BF), pltpu.VMEM(by_gate.shape, BF), pltpu.VMEM(act.shape, BF), pltpu.VMEM(by_out.shape, BF)]
    scratch += [pltpu.VMEM((4, 8, 128), F32), pltpu.VMEM((4, 4, 8, 128), F32), pltpu.SemaphoreType.DMA((1300,))]
    (D, tokens), FF = a.shape, act.shape[0]
    outs = [(2, 16, 56, FF), (2, 16, 56, FF), (2, 32, 72, D)]
    *sums, squares = pl.pallas_call(
        reduce_kernel,
        out_shape=[jax.ShapeDtypeStruct(shape, BF) for shape in outs] + [jax.ShapeDtypeStruct((8, 128), F32)],
        in_specs=[pl.BlockSpec(memory_space=pltpu.HBM)] * 10,
        out_specs=[pl.BlockSpec(memory_space=pltpu.HBM)] * 3 + [pl.BlockSpec(memory_space=pltpu.VMEM)],
        scratch_shapes=scratch,
        compiler_params=pltpu.CompilerParams(collective_id=0, has_side_effects=True, vmem_limit_bytes=67_043_328),
    )(*layers[0], *layers[1])
    return [s.reshape(2, -1, s.shape[-1]) for s in sums], squares


TOKENS = 512
CHUNK = 256


def mm(a, w, contract):
    return lax.dot_general(a, w, ((contract[0], contract[1]), ((), ())), preferred_element_type=F32)


def scale_of(wide):
    return lax.rsqrt(jnp.mean(wide * wide, -1, keepdims=True) + 1e-6)


def gates(gate, up, by_act):
    s = jax.nn.sigmoid(gate)
    silu = gate * s
    by_act = by_act.astype(F32)
    return (silu * up).astype(BF), (by_act * up * (s + silu * (1 - s))).astype(BF), (by_act * silu).astype(BF)


def chain_kernel(x, dy, wg_hbm, wu_hbm, wd_hbm, a1_t, dg1, du1, act1_t, dh1, a2_t, dg2, du2, act2_t, wg, wu, wd, gate1, up1, a1, a2, act1, sem):
    first = pl.program_id(0) == 0
    copies = [
        pltpu.make_async_copy(hbm.at[l], vmem.at[l], sem.at[n])
        for n, (hbm, vmem, l) in enumerate(
            (hbm, vmem, l) for l in range(2) for hbm, vmem in ((wg_hbm, wg), (wu_hbm, wu), (wd_hbm, wd))
        )
    ]

    @pl.when(first)
    def _():
        for copy in copies:
            copy.start()

    def ready(*numbers):
        @pl.when(first)
        def _():
            for n in numbers:
                copies[n].wait()

    FF, D = wd.shape[1:]

    def chunks(body):
        for n in range(0, FF, CHUNK):
            body(slice(n, n + CHUNK))

    columns = [slice(n, min(n + 256, D)) for n in range(0, D, 256)]
    nn, nt = ((1,), (0,)), ((1,), (1,))

    wide = x[...].astype(F32)
    a = wide * scale_of(wide)
    a1[...] = a.astype(BF)
    a1_t[...] = a.astype(BF).T
    ready(0, 1)

    def forward1(c):
        gate = mm(a1[...], wg[0, :, c], nn)
        up = mm(a1[...], wu[0, :, c], nn)
        gate1[:, c] = gate
        up1[:, c] = up
        act = (jax.nn.silu(gate) * up).astype(BF)
        act1[:, c] = act
        act1_t[c, :] = act.T

    lax.fori_loop(0, FF // CHUNK, lambda i, c: (forward1(pl.ds(pl.multiple_of(i * CHUNK, CHUNK), CHUNK)), c)[1], 0)
    ready(2)
    for n in columns:
        dh1[:, n] = x[:, n] + mm(act1[...], wd[0, :, n], nn).astype(BF)
    wide = dh1[...].astype(F32)
    a = wide * scale_of(wide)
    a2[...] = a.astype(BF)
    a2_t[...] = a.astype(BF).T
    ready(3, 4, 5)

    def both2(c):
        gate = mm(a2[...], wg[1, :, c], nn)
        up = mm(a2[...], wu[1, :, c], nn)
        by_act = mm(dy[...], wd[1, c, :], nt).astype(BF)
        act, dg2[:, c], du2[:, c] = gates(gate, up, by_act)
        act2_t[c, :] = act.T

    chunks(both2)
    by_a = []
    for n in columns:
        by_a.append((mm(dg2[...], wg[1, n, :], nt).astype(BF) + mm(du2[...], wu[1, n, :], nt).astype(BF)).astype(F32))
    by_a = jnp.concatenate(by_a, -1)
    wide = dh1[...].astype(F32)
    scale = scale_of(wide)
    by_scale = jnp.sum(by_a * wide, -1, keepdims=True)
    by_h = by_a * scale - wide * (by_scale * scale * scale * scale * (1 / D))
    dh1[...] = dy[...] + by_h.astype(BF)

    def backward1(c):
        by_act = mm(dh1[...], wd[0, c, :], nt).astype(BF)
        _, dg1[:, c], du1[:, c] = gates(gate1[:, c], up1[:, c], by_act)

    chunks(backward1)


def chain(x, dy, w_gate, w_up, w_down):
    tokens, D = x.shape
    FF = w_down.shape[1]

    def across(width):
        return pl.BlockSpec((TOKENS, width), lambda i: (i, 0), pipeline_mode=pl.Buffered(1)), jax.ShapeDtypeStruct((tokens, width), BF)

    def along(width):
        return pl.BlockSpec((width, TOKENS), lambda i: (0, i), pipeline_mode=pl.Buffered(1)), jax.ShapeDtypeStruct((width, tokens), BF)

    layer = [along(D), across(FF), across(FF), along(FF)]
    out_specs, out_shape = zip(*layer, across(D), *layer, strict=True)
    *ones, dh1, a2_t, dg2, du2, act2_t = pl.pallas_call(
        chain_kernel,
        grid=(tokens // TOKENS,),
        in_specs=[pl.BlockSpec((TOKENS, D), lambda i: (i, 0))] * 2 + [pl.BlockSpec(memory_space=pltpu.HBM)] * 3,
        out_specs=out_specs,
        out_shape=out_shape,
        scratch_shapes=[
            pltpu.VMEM(w_gate.shape, BF),
            pltpu.VMEM(w_up.shape, BF),
            pltpu.VMEM(w_down.shape, BF),
            pltpu.VMEM((TOKENS, FF), F32),
            pltpu.VMEM((TOKENS, FF), F32),
            pltpu.VMEM((TOKENS, D), BF),
            pltpu.VMEM((TOKENS, D), BF),
            pltpu.VMEM((TOKENS, FF), BF),
            pltpu.SemaphoreType.DMA((6,)),
        ],
        compiler_params=pltpu.CompilerParams(vmem_limit_bytes=67_000_000),
    )(x, dy, w_gate, w_up, w_down)
    return (*ones, dh1), (a2_t, dg2, du2, act2_t, dy)


COUNT = 2 * 3 * 896 * 2304


def adamw_kernel(squares, *refs):
    ins, outs, factor = refs[:12], refs[12:21], refs[21]

    @pl.when((pl.program_id(0) == 0) & (pl.program_id(1) == 0))
    def _():
        whole = 0.25 * jnp.sum(squares[...])
        factor[0] = jnp.minimum(1.0, 0.5 * lax.rsqrt(whole / COUNT + 1e-30))

    by = factor[0]
    for k in range(3):
        w, m, v, g = (ins[i * 3 + k] for i in range(4))

        rows = w.shape[1] // (2 if k < 2 else 4)

        def some(i, carry):
            to = pl.ds(pl.multiple_of(i * rows, 8), rows)
            grad = g[0, to].astype(F32) * by
            new_m = 0.9 * m[0, to] + 0.1 * grad
            new_v = 0.95 * v[0, to] + 0.05 * grad * grad
            wide = w[0, to].astype(F32)
            step = new_m * lax.rsqrt(new_v + 1e-8) + 0.1 * wide
            outs[k][0, to] = (wide - 0.02 * step).astype(BF)
            outs[3 + k][0, to] = new_m
            outs[6 + k][0, to] = new_v
            return carry

        lax.fori_loop(0, w.shape[1] // rows, some, 0)


def adamw(weights, m, v, gradients, squares):
    layers = weights[0].shape[0]
    spec = lambda w: pl.BlockSpec((1, w.shape[1] // 8, w.shape[2]), lambda l, i: (l, i, 0))
    specs = [spec(w) for w in weights]
    return pl.pallas_call(
        adamw_kernel,
        grid=(layers, 8),
        in_specs=[pl.BlockSpec(memory_space=pltpu.VMEM)] + specs * 4,
        out_specs=specs * 3,
        out_shape=[jax.ShapeDtypeStruct(w.shape, t) for t in (BF, F32, F32) for w in weights],
        scratch_shapes=[pltpu.SMEM((1,), F32)],
        compiler_params=pltpu.CompilerParams(vmem_limit_bytes=60_000_000),
    )(squares, *weights, *m, *v, *gradients)


def solution(mesh):
    def step(x, dy, *arrays):
        weights, m, v = (arrays[i : i + 3] for i in (0, 3, 6))
        gradients, squares = summed(chain(x[0], dy[0], *weights))
        return tuple(adamw(weights, m, v, gradients, squares))

    return jax.shard_map(
        step,
        mesh=mesh,
        in_specs=(P(("rep", "dp"), None, None),) * 2 + (P(None, None, None),) * 9,
        out_specs=(P("rep", None, None),) * 9,
        check_vma=False,
    )
```

```python
import functools

import jax
import jax.numpy as jnp
from jax import lax
from jax.experimental import pallas as pl
from jax.experimental.pallas import tpu as pltpu
from jax.sharding import PartitionSpec as P

BF, F32 = jnp.bfloat16, jnp.float32
BLOCK = ((56, 1152), (56, 1152), (72, 896))
UPWARD = 32
AXES = ((0, 1, 2), (1, 2, 0), (2, 0, 1))
SLOT = 6.0
GAPS = (6, 6, 6, 5, 6, 6, 8, 8)


class Sems:
    def __init__(self, ref):
        self.ref, self.used = ref, 0

    def __call__(self):
        self.used += 1
        return self.ref.at[self.used - 1]


def reduce_kernel(*refs):
    ins = [refs[l * 5 : l * 5 + 5] for l in range(2)]
    outs, ss_out = refs[10:13], refs[13]
    it = iter(refs[14:-7])
    own, far, q1, q2, via, v1, v2, uvia, x, fin = ([[next(it) for _ in range(3)] for _ in range(2)] for _ in range(10))
    f, t, theirs = ([each] * 2 for each in ([next(it) for _ in range(3)] for _ in range(3)))
    tall, broad, deep, flat, ss, ssx, sem_ref = refs[-7:]
    sem = Sems(sem_ref)

    me = lax.axis_index("dp")
    core = lax.rem(me, 2)
    pos = [lax.rem(me // 32, 4), lax.rem(me // 8, 4), lax.rem(me // 2, 4)]
    stride = (32, 8, 2)

    def turn(place, by):
        return lax.rem(place + by, 4)

    def at(axis, by):
        return me + (turn(pos[axis], by) - pos[axis]) * stride[axis]

    partner = me + 1 - 2 * core

    def dev(index):
        return (0, index)

    def part(ref, k, half, first, n, rows=slice(None)):
        if k < 2:
            return ref.at[pl.ds(first, n), rows, pl.ds(pl.multiple_of(half * 1152, 128), 1152)]
        return ref.at[pl.ds(half * 16 + first, n), rows, :]

    pending = []

    def send(src, dst, to):
        copy = pltpu.make_async_remote_copy(
            src_ref=src, dst_ref=dst, send_sem=sem(), recv_sem=sem(), device_id=dev(to), device_id_type=pl.DeviceIdType.MESH
        )
        copy.start()
        pending.append(copy)
        return copy

    friends = [partner] + [at(a, by) for a in range(3) for by in (1, 2, 3)]

    def sent(copy):
        copy.wait_send()
        pending[:] = [each for each in pending if each is not copy]

    got = {}
    order = [(l, k) for l in (1, 0) for k in range(3)]

    def blocks(n, body):
        lax.fori_loop(0, n, lambda i, c: (body(i), c)[1], 0)

    def wide(ref, i):
        return ref[i].astype(F32)

    loads = {}

    def load(name, l, which, dst):
        loads[name, l] = pltpu.make_async_copy(ins[l][which], dst, sem())
        loads[name, l].start()

    def s0(n, by):
        l, k = order[n]
        first = turn(pos[AXES[k][0]], by) * 4
        rows, cols = BLOCK[k]
        if by == 2:
            for name in (("tall", "gate"), ("up",), ("deep", "flat"))[k]:
                loads[name, l].wait()
        if l == 0:
            sent(got[1, k, "far", by])
        for half, to in ((core, own[l][k]), (1 - core, theirs[l][k])):
            if k < 2:
                lhs = tall[pl.ds(pl.multiple_of(first * rows, 8), 4 * rows), :]
                rhs = broad[:, pl.ds(pl.multiple_of(half * 1152, 128), 1152)]
            else:
                lhs = deep[pl.ds(pl.multiple_of(half * 1152 + first * rows, 8), 4 * rows), :]
                rhs = flat[...]
            to[pl.ds(first, 4)] = jnp.dot(lhs, rhs, preferred_element_type=F32).reshape(4, rows, cols).astype(BF)
        got[l, k, "far", by] = send(theirs[l][k].at[pl.ds(first, 4)], far[l][k].at[pl.ds(first, 4)], partner)
        if by == 0:
            if k == 0:
                load("up", l, 2, broad)
            elif n == 1:
                load("tall", 0, 0, tall)
                load("gate", 0, 1, broad)
            elif n == 2:
                load("deep", 0, 3, deep)
                load("flat", 0, 4, flat)

    def both(l, k, by):
        got[l, k, "far", by].wait_recv()

    def presum(l, k, first, n):
        def body(i):
            own[l][k][first + i] = (wide(own[l][k], first + i) + wide(far[l][k], first + i)).astype(BF)

        blocks(n, body)

    def s1(l, k):
        a = AXES[k][0]
        p = pos[a]
        both(l, k, 2)
        b = turn(p, 2) * 4
        presum(l, k, b, 4)
        got[l, k, "1p"] = send(own[l][k].at[pl.ds(b, 2)], via[l][k].at[0], at(a, 1))
        got[l, k, "1m"] = send(own[l][k].at[pl.ds(b + 2, 2)], via[l][k].at[1], at(a, 3))

    def s2(l, k):
        a = AXES[k][0]
        p = pos[a]
        both(l, k, 1)
        b = turn(p, 1) * 4 + 2
        presum(l, k, b, 2)
        got[l, k, "2p"] = send(own[l][k].at[pl.ds(b, 2)], q1[l][k].at[pl.ds(2, 2)], at(a, 1))
        both(l, k, 3)
        b = turn(p, 3) * 4
        presum(l, k, b, 2)
        got[l, k, "2m"] = send(own[l][k].at[pl.ds(b, 2)], q1[l][k].at[pl.ds(0, 2)], at(a, 3))

    def s3(l, k):
        a = AXES[k][0]
        p = pos[a]
        for way, by, half in ((0, 1, 0), (1, 3, 2)):
            got[l, k, "1" + "pm"[way]].wait_recv()
            b = turn(p, by) * 4 + half

            def body(i):
                own[l][k][b + i] = (wide(own[l][k], b + i) + wide(far[l][k], b + i) + via[l][k][way, i].astype(F32)).astype(BF)

            blocks(2, body)
            got[l, k, "3" + "pm"[way]] = send(own[l][k].at[pl.ds(b, 2)], q2[l][k].at[pl.ds(half, 2)], at(a, by))

    up, down = slice(0, UPWARD), slice(UPWARD, None)
    aheads = (("p", 1), ("m", 3))
    ways = (("p", 3, up, 1), ("m", 1, down, 3))

    def s4(l, k):
        a, a2 = AXES[k][:2]
        p, q = pos[a], pos[a2]
        both(l, k, 0)
        for name in ("2p", "2m", "3p", "3m"):
            got[l, k, name].wait_recv()

        def body(i):
            j = turn(q, 2 + i)
            whole = wide(own[l][k], p * 4 + j) + wide(far[l][k], p * 4 + j) + wide(q1[l][k], j) + wide(q2[l][k], j)
            f[l][k][i] = whole
            t[l][k][i] = whole.astype(BF)

        if l == 0:
            for name in ("u1p", "u1m", "u2p", "u2m", "u3p", "u3m"):
                sent(got[1, k, name])

        blocks(4, body)
        got[l, k, "u1p"] = send(t[l][k].at[0, up], uvia[l][k].at[up], at(a2, 1))
        got[l, k, "u1m"] = send(t[l][k].at[0, down], uvia[l][k].at[down], at(a2, 3))
        got[l, k, "u2p"] = send(t[l][k].at[3, down], v1[l][k].at[down], at(a2, 1))
        got[l, k, "u2m"] = send(t[l][k].at[1, up], v1[l][k].at[up], at(a2, 3))

    def s5(l, k):
        a2 = AXES[k][1]
        got[l, k, "u1p"].wait_recv()
        t[l][k][3, up] = (f[l][k][3, up] + uvia[l][k][up].astype(F32)).astype(BF)
        got[l, k, "u3p"] = send(t[l][k].at[3, up], v2[l][k].at[up], at(a2, 1))
        got[l, k, "u1m"].wait_recv()
        t[l][k][1, down] = (f[l][k][1, down] + uvia[l][k][down].astype(F32)).astype(BF)
        got[l, k, "u3m"] = send(t[l][k].at[1, down], v2[l][k].at[down], at(a2, 3))

    def s6(l, k):
        a3 = AXES[k][2]
        r = pos[a3]
        for name in ("u2p", "u2m", "u3p", "u3m"):
            got[l, k, name].wait_recv()
        x[l][k][r] = (f[l][k][2] + v1[l][k][...].astype(F32) + v2[l][k][...].astype(F32)).astype(BF)
        got[l, k, "x1p"] = send(x[l][k].at[r], x[l][k].at[r], at(a3, 1))
        got[l, k, "x1m"] = send(x[l][k].at[r], x[l][k].at[r], at(a3, 3))

    def s7(l, k):
        a3 = AXES[k][2]
        r = pos[a3]
        got[l, k, "x1p"].wait_recv()
        b = turn(r, 3)
        got[l, k, "x2p"] = send(x[l][k].at[b, up], x[l][k].at[b, up], at(a3, 1))
        got[l, k, "x1m"].wait_recv()
        b = turn(r, 1)
        got[l, k, "x2m"] = send(x[l][k].at[b, down], x[l][k].at[b, down], at(a3, 3))

    def place(l, k, half, first, n, rows=slice(None)):
        return part(outs[k].at[l], k, half, first, n, rows)

    def s8(l, k):
        a, a2 = AXES[k][:2]
        p, q = pos[a], pos[a2]
        got[l, k, "x2p"].wait_recv()
        got[l, k, "x2m"].wait_recv()
        whole = (x[l][k][0].astype(F32) + x[l][k][1].astype(F32)) + (x[l][k][2].astype(F32) + x[l][k][3].astype(F32))
        g = whole.astype(BF)
        fin[l][k][0] = g
        mine = p * 4 + q
        copy = pltpu.make_async_copy(fin[l][k], place(l, k, core, mine, 1), sem())
        copy.start()
        got[l, k, "mine"] = copy
        got[l, k, "y1p"] = send(fin[l][k], place(l, k, core, mine, 1), at(a2, 1))
        got[l, k, "y1m"] = send(fin[l][k], place(l, k, core, mine, 1), at(a2, 3))
        got[l, k, "z1p", 0] = send(fin[l][k], place(l, k, core, mine, 1), at(a, 1))
        got[l, k, "z1m", 0] = send(fin[l][k], place(l, k, core, mine, 1), at(a, 3))
        wide_g = g.astype(F32)
        squares = wide_g * wide_g
        rows, cols = BLOCK[k]
        by_row = sum(squares[i : i + 8] for i in range(0, rows, 8))
        return sum(by_row[:, i : i + 128] for i in range(0, cols, 128))

    def s9(l, k):
        a, a2 = AXES[k][:2]
        p, q = pos[a], pos[a2]
        for name, by, rows, to in ways:
            got[l, k, "y1" + name].wait_recv()
            b = p * 4 + turn(q, by)
            got[l, k, "y2" + name] = send(place(l, k, core, b, 1, rows), place(l, k, core, b, 1, rows), at(a2, to))
            for way, ahead in aheads:
                got[l, k, "z1" + way, by] = send(place(l, k, core, b, 1), place(l, k, core, b, 1), at(a, ahead))

    def onward(l, k, d):
        a, a2 = AXES[k][:2]
        p, q = pos[a], pos[a2]
        j = turn(q, d)
        for name, by, rows, to in ways:
            got[l, k, "z1" + name, d].wait_recv()
            b = turn(p, by) * 4 + j
            got[l, k, "z2" + name, d] = send(place(l, k, core, b, 1, rows), place(l, k, core, b, 1, rows), at(a, to))

    def s10(l, k):
        a, a2 = AXES[k][:2]
        p, q = pos[a], pos[a2]
        got[l, k, "y2p"].wait_recv()
        got[l, k, "y2m"].wait_recv()
        b = p * 4 + turn(q, 2)
        for way, ahead in aheads:
            got[l, k, "z1" + way, 2] = send(place(l, k, core, b, 1), place(l, k, core, b, 1), at(a, ahead))
        got[l, k, "mine"].wait()
        got[l, k, "c", 0] = send(place(l, k, core, p * 4, 4), place(l, k, core, p * 4, 4), partner)
        onward(l, k, 0)

    def s11(l, k):
        for d in (3, 1, 2):
            onward(l, k, d)
        p = pos[AXES[k][0]]
        for by in (1, 3):
            b = turn(p, by) * 4
            got[l, k, "c", by] = send(place(l, k, core, b, 4), place(l, k, core, b, 4), partner)

    def s12(l, k):
        for d in range(4):
            got[l, k, "z2p", d].wait_recv()
            got[l, k, "z2m", d].wait_recv()
        b = turn(pos[AXES[k][0]], 2) * 4
        got[l, k, "c", 2] = send(place(l, k, core, b, 4), place(l, k, core, b, 4), partner)

    rounds = [(2, core, [partner])] + [(4, pos[a], [at(a, by) for by in (1, 2, 3)]) for a in range(3)]
    squares, arrivals = [], []

    def add_squares(number):
        total = squares[-1] if number else sum(squares)
        if number:
            for arrival in arrivals.pop():
                arrival.wait_recv()
            total = ssx[number - 1, 0] + ssx[number - 1, 1]
            if number > 1:
                total = total + (ssx[number - 1, 2] + ssx[number - 1, 3])
        if number == 4:
            ss_out[...] = total
            return
        _, spot, others = rounds[number]
        ss[number] = total
        ssx[number, spot] = total
        arrivals.append([send(ss.at[number], ssx.at[number, spot], to) for to in others])

    plan = []
    for n, (l, k) in enumerate(order):
        one = SLOT * n
        for number, by in enumerate((2, 1, 3, 0)):
            plan.append((one + number * SLOT / 4, s0, (n, by)))
        times = [one + 0.45 * SLOT, one + 0.95 * SLOT, one + 0.45 * SLOT + 7]
        times.append(one + 0.45 * SLOT + 19)
        for gap in GAPS:
            times.append(times[-1] + gap)
        for stage, time in zip((s1, s2, s3, s4, s5, s6, s7, s8, s9, s10, s11, s12), times, strict=True):
            plan.append((time, stage, (l, k)))
    last = max(time for time, stage, _ in plan if stage is s8)
    plan += [(last + 0.1 + 3 * number, add_squares, (number,)) for number in range(5)]
    for name, which, dst in (("tall", 0, tall), ("gate", 1, broad), ("deep", 3, deep), ("flat", 4, flat)):
        load(name, 1, which, dst)
    barrier = pltpu.get_barrier_semaphore()
    for friend in friends:
        pl.semaphore_signal(barrier, inc=1, device_id=dev(friend), device_id_type=pl.DeviceIdType.MESH)
    pl.semaphore_wait(barrier, len(friends))
    for _, stage, which in sorted(plan, key=lambda entry: entry[0]):
        result = stage(*which)
        if stage is s8:
            squares.append(result)
    for l, k in order:
        for by in range(4):
            got[l, k, "c", by].wait_recv()
    for copy in pending:
        copy.wait_send()


def summed(layers):
    scratch = []
    per = lambda shape, dtype, count: [pltpu.VMEM(shape(*BLOCK[k]), dtype) for _ in range(count) for k in range(3)]
    for shape, dtype, count in (
        (lambda r, c: (16, r, c), BF, 2),
        (lambda r, c: (16, r, c), BF, 2),
        (lambda r, c: (4, r, c), BF, 2),
        (lambda r, c: (4, r, c), BF, 2),
        (lambda r, c: (2, 2, r, c), BF, 2),
        (lambda r, c: (r, c), BF, 2),
        (lambda r, c: (r, c), BF, 2),
        (lambda r, c: (r, c), BF, 2),
        (lambda r, c: (4, r, c), BF, 2),
        (lambda r, c: (1, r, c), BF, 2),
        (lambda r, c: (4, r, c), F32, 1),
        (lambda r, c: (4, r, c), BF, 1),
        (lambda r, c: (16, r, c), BF, 1),
    ):
        scratch += per(shape, dtype, count)
    a, by_gate, _, act, by_out = layers[0]
    scratch += [pltpu.VMEM(a.shape, BF), pltpu.VMEM(by_gate.shape, BF), pltpu.VMEM(act.shape, BF), pltpu.VMEM(by_out.shape, BF)]
    scratch += [pltpu.VMEM((4, 8, 128), F32), pltpu.VMEM((4, 4, 8, 128), F32), pltpu.SemaphoreType.DMA((640,))]
    (D, tokens), FF = a.shape, act.shape[0]
    outs = [(2, 16, 56, FF), (2, 16, 56, FF), (2, 32, 72, D)]
    *sums, squares = pl.pallas_call(
        reduce_kernel,
        out_shape=[jax.ShapeDtypeStruct(shape, BF) for shape in outs] + [jax.ShapeDtypeStruct((8, 128), F32)],
        in_specs=[pl.BlockSpec(memory_space=pltpu.HBM)] * 10,
        out_specs=[pl.BlockSpec(memory_space=pltpu.HBM)] * 3 + [pl.BlockSpec(memory_space=pltpu.VMEM)],
        scratch_shapes=scratch,
        compiler_params=pltpu.CompilerParams(collective_id=0, has_side_effects=True, vmem_limit_bytes=67_043_328),
    )(*layers[0], *layers[1])
    return [s.reshape(2, -1, s.shape[-1]) for s in sums], squares


TOKENS = 512
CHUNK = 256


def mm(a, w, contract):
    return lax.dot_general(a, w, ((contract[0], contract[1]), ((), ())), preferred_element_type=F32)


def scale_of(wide):
    return lax.rsqrt(jnp.mean(wide * wide, -1, keepdims=True) + 1e-6)


def gates(gate, up, by_act):
    s = jax.nn.sigmoid(gate)
    silu = gate * s
    by_act = by_act.astype(F32)
    return (silu * up).astype(BF), (by_act * up * (s + silu * (1 - s))).astype(BF), (by_act * silu).astype(BF)


def chain_kernel(x, dy, wg_hbm, wu_hbm, wd_hbm, a1_t, dg1, du1, act1_t, dh1, a2_t, dg2, du2, act2_t, wg, wu, wd, gate1, up1, a1, a2, act1, sem):
    first = pl.program_id(0) == 0
    copies = [
        pltpu.make_async_copy(hbm.at[l], vmem.at[l], sem.at[n])
        for n, (hbm, vmem, l) in enumerate(
            (hbm, vmem, l) for l in range(2) for hbm, vmem in ((wg_hbm, wg), (wu_hbm, wu), (wd_hbm, wd))
        )
    ]

    @pl.when(first)
    def _():
        for copy in copies:
            copy.start()

    def ready(*numbers):
        @pl.when(first)
        def _():
            for n in numbers:
                copies[n].wait()

    FF, D = wd.shape[1:]

    def chunks(body):
        for n in range(0, FF, CHUNK):
            body(slice(n, n + CHUNK))

    columns = [slice(n, min(n + 256, D)) for n in range(0, D, 256)]
    nn, nt = ((1,), (0,)), ((1,), (1,))

    wide = x[...].astype(F32)
    a = wide * scale_of(wide)
    a1[...] = a.astype(BF)
    a1_t[...] = a.astype(BF).T
    ready(0, 1)

    def forward1(c):
        gate = mm(a1[...], wg[0, :, c], nn)
        up = mm(a1[...], wu[0, :, c], nn)
        gate1[:, c] = gate
        up1[:, c] = up
        act = (jax.nn.silu(gate) * up).astype(BF)
        act1[:, c] = act
        act1_t[c, :] = act.T

    chunks(forward1)
    ready(2)
    for n in columns:
        dh1[:, n] = x[:, n] + mm(act1[...], wd[0, :, n], nn).astype(BF)
    wide = dh1[...].astype(F32)
    a = wide * scale_of(wide)
    a2[...] = a.astype(BF)
    a2_t[...] = a.astype(BF).T
    ready(3, 4, 5)

    def both2(c):
        gate = mm(a2[...], wg[1, :, c], nn)
        up = mm(a2[...], wu[1, :, c], nn)
        by_act = mm(dy[...], wd[1, c, :], nt).astype(BF)
        act, dg2[:, c], du2[:, c] = gates(gate, up, by_act)
        act2_t[c, :] = act.T

    chunks(both2)
    by_a = []
    for n in columns:
        by_a.append((mm(dg2[...], wg[1, n, :], nt).astype(BF) + mm(du2[...], wu[1, n, :], nt).astype(BF)).astype(F32))
    by_a = jnp.concatenate(by_a, -1)
    wide = dh1[...].astype(F32)
    scale = scale_of(wide)
    by_scale = jnp.sum(by_a * wide, -1, keepdims=True)
    by_h = by_a * scale - wide * (by_scale * scale * scale * scale * (1 / D))
    dh1[...] = dy[...] + by_h.astype(BF)

    def backward1(c):
        by_act = mm(dh1[...], wd[0, c, :], nt).astype(BF)
        _, dg1[:, c], du1[:, c] = gates(gate1[:, c], up1[:, c], by_act)

    chunks(backward1)


def chain(x, dy, w_gate, w_up, w_down):
    tokens, D = x.shape
    FF = w_down.shape[1]

    def across(width):
        return pl.BlockSpec((TOKENS, width), lambda i: (i, 0), pipeline_mode=pl.Buffered(1)), jax.ShapeDtypeStruct((tokens, width), BF)

    def along(width):
        return pl.BlockSpec((width, TOKENS), lambda i: (0, i), pipeline_mode=pl.Buffered(1)), jax.ShapeDtypeStruct((width, tokens), BF)

    layer = [along(D), across(FF), across(FF), along(FF)]
    out_specs, out_shape = zip(*layer, across(D), *layer, strict=True)
    *ones, dh1, a2_t, dg2, du2, act2_t = pl.pallas_call(
        chain_kernel,
        grid=(tokens // TOKENS,),
        in_specs=[pl.BlockSpec((TOKENS, D), lambda i: (i, 0))] * 2 + [pl.BlockSpec(memory_space=pltpu.HBM)] * 3,
        out_specs=out_specs,
        out_shape=out_shape,
        scratch_shapes=[
            pltpu.VMEM(w_gate.shape, BF),
            pltpu.VMEM(w_up.shape, BF),
            pltpu.VMEM(w_down.shape, BF),
            pltpu.VMEM((TOKENS, FF), F32),
            pltpu.VMEM((TOKENS, FF), F32),
            pltpu.VMEM((TOKENS, D), BF),
            pltpu.VMEM((TOKENS, D), BF),
            pltpu.VMEM((TOKENS, FF), BF),
            pltpu.SemaphoreType.DMA((6,)),
        ],
        compiler_params=pltpu.CompilerParams(vmem_limit_bytes=67_000_000),
    )(x, dy, w_gate, w_up, w_down)
    return (*ones, dh1), (a2_t, dg2, du2, act2_t, dy)


COUNT = 2 * 3 * 896 * 2304


def adamw_kernel(squares, *refs):
    ins, outs, factor = refs[:12], refs[12:21], refs[21]

    @pl.when((pl.program_id(0) == 0) & (pl.program_id(1) == 0))
    def _():
        whole = 0.25 * jnp.sum(squares[...])
        factor[0] = jnp.minimum(1.0, 0.5 * lax.rsqrt(whole / COUNT + 1e-30))

    by = factor[0]
    for k in range(3):
        w, m, v, g = (ins[i * 3 + k] for i in range(4))

        rows = w.shape[1] // (2 if k < 2 else 4)

        def some(i, carry):
            to = pl.ds(pl.multiple_of(i * rows, 8), rows)
            grad = g[0, to].astype(F32) * by
            new_m = 0.9 * m[0, to] + 0.1 * grad
            new_v = 0.95 * v[0, to] + 0.05 * grad * grad
            wide = w[0, to].astype(F32)
            step = new_m * lax.rsqrt(new_v + 1e-8) + 0.1 * wide
            outs[k][0, to] = (wide - 0.02 * step).astype(BF)
            outs[3 + k][0, to] = new_m
            outs[6 + k][0, to] = new_v
            return carry

        lax.fori_loop(0, w.shape[1] // rows, some, 0)


def adamw(weights, m, v, gradients, squares):
    layers = weights[0].shape[0]
    spec = lambda w: pl.BlockSpec((1, w.shape[1] // 8, w.shape[2]), lambda l, i: (l, i, 0))
    specs = [spec(w) for w in weights]
    return pl.pallas_call(
        adamw_kernel,
        grid=(layers, 8),
        in_specs=[pl.BlockSpec(memory_space=pltpu.VMEM)] + specs * 4,
        out_specs=specs * 3,
        out_shape=[jax.ShapeDtypeStruct(w.shape, t) for t in (BF, F32, F32) for w in weights],
        scratch_shapes=[pltpu.SMEM((1,), F32)],
        compiler_params=pltpu.CompilerParams(vmem_limit_bytes=60_000_000),
    )(squares, *weights, *m, *v, *gradients)


def solution(mesh):
    def step(x, dy, *arrays):
        weights, m, v = (arrays[i : i + 3] for i in (0, 3, 6))
        gradients, squares = summed(chain(x[0], dy[0], *weights))
        return tuple(adamw(weights, m, v, gradients, squares))

    return jax.shard_map(
        step,
        mesh=mesh,
        in_specs=(P(("rep", "dp"), None, None),) * 2 + (P(None, None, None),) * 9,
        out_specs=(P("rep", None, None),) * 9,
        check_vma=False,
    )
```
